16 devices in a mesh: dp: 1, sp: 16 (over x, y, z, core).
Axes of the slice: x: 2, y: 2, z: 2, core: 2. Of those that a mesh axis runs over, the one named last changes fastest.
Arguments:
- x: bfloat16 [2048, 12288], P(('dp', 'sp'))
- gain: bfloat16 [12288], replicated
- wq: bfloat16 [12288, 12288], replicated
- wk: bfloat16 [12288, 12288], replicated
- wv: bfloat16 [12288, 12288], replicated
- wo: bfloat16 [12288, 12288], replicated
Outputs:
- output: bfloat16 [2048, 12288], P(('dp', 'sp'))
All inputs are finite; a program needn't handle non-finite values.
Results may differ from the reference program's by a relative error of at most 0.012.
Values are sent between devices in bfloat16 or wider.
A program may use at most 2.75 GiB of HBM per device.

```python
import jax
import jax.numpy as jnp
from jax import lax

ROWS = 2048
D = 12288
HEADS = 96
KV_HEADS = 96
HEAD = 128
THETA = 10000


def setup_inputs(seed: int = 0, part: int = 0) -> dict:
    kx, kn, kq, kk, kv, ko = jax.random.split(jax.random.key(seed), 6)

    def weights(key, rows, columns):
        return jax.random.normal(key, (rows, columns), jnp.float32) * rows**-0.5

    drawn = {
        "x": jax.random.normal(jax.random.fold_in(kx, part), (ROWS, D), jnp.float32),
        "gain": 1 + 0.1 * jax.random.normal(kn, (D,), jnp.float32),
        "wq": 2 * weights(kq, D, HEADS * HEAD),
        "wk": 2 * weights(kk, D, KV_HEADS * HEAD),
        "wv": 4 * weights(kv, D, KV_HEADS * HEAD),
        "wo": weights(ko, HEADS * HEAD, D),
    }
    return {k: v.astype(jnp.bfloat16) for k, v in drawn.items()}


def normed(x, gain):
    wide = x.astype(jnp.float32)
    scale = lax.rsqrt(jnp.mean(wide * wide, -1, keepdims=True) + 1e-6)
    return (wide * scale * gain.astype(jnp.float32)).astype(jnp.bfloat16)


def turned(t, place, theta):
    half = t.shape[-1] // 2
    angle = place.astype(jnp.float32)[:, None] * theta ** (-jnp.arange(half, dtype=jnp.float32) / half)
    cos, sin = jnp.cos(angle)[:, None], jnp.sin(angle)[:, None]
    a, b = t[..., :half].astype(jnp.float32), t[..., half:].astype(jnp.float32)
    return jnp.concatenate([a * cos - b * sin, b * cos + a * sin], -1).astype(jnp.bfloat16)


def matmul(a, w):
    return jnp.dot(a, w, preferred_element_type=jnp.float32).astype(jnp.bfloat16)


def einsum(form, a, b):
    return jnp.einsum(form, a.astype(jnp.float32), b.astype(jnp.float32))


def attention(q, k, v):
    scores = einsum("tgsd,ugd->gstu", q, k) * q.shape[-1] ** -0.5
    token = jnp.arange(q.shape[0])
    scores = jnp.where(token[:, None] >= token, scores, -jnp.inf)
    weights = jax.nn.softmax(scores, -1).astype(jnp.bfloat16)
    return einsum("gstu,ugd->tgsd", weights, v).astype(jnp.bfloat16)


def reference(x, gain, wq, wk, wv, wo):
    a, place = normed(x, gain), jnp.arange(ROWS)
    q = turned(matmul(a, wq).reshape(ROWS, HEADS, HEAD), place, THETA).reshape(ROWS, KV_HEADS, -1, HEAD)
    k = turned(matmul(a, wk).reshape(ROWS, KV_HEADS, HEAD), place, THETA)
    v = matmul(a, wv).reshape(ROWS, KV_HEADS, HEAD)
    seen = attention(q, k, v).reshape(ROWS, HEADS * HEAD)
    return (x.astype(jnp.float32) + jnp.dot(seen, wo, preferred_element_type=jnp.float32)).astype(jnp.bfloat16)
```

```python
import functools

import jax
import jax.numpy as jnp
from jax import lax
from jax.experimental import pallas as pl
from jax.experimental.pallas import tpu as pltpu
from jax.sharding import PartitionSpec as P

HEAD = 128
THETA = 10000
NEG = -1e30
HIDDEN = 2 * NEG
LOG2E = 1.4426950408889634
D = 12288
HALF = D // 2
CHIPS = 8
TOK = 256
W = 256
PASSES = 3
SLOTS = 4
KB = 512


def _dot(a, b, ca, cb):
    return lax.dot_general(a, b, (((ca,), (cb,)), ((), ())), preferred_element_type=jnp.float32)


def _kernel(x_ref, gain_ref, cos_ref, sin_ref, wq_ref, wk_ref, wv_ref, wo_ref, y_ref,
            a_s, xres, ring, qkv, stage, seen, yacc, top_s, mix_s,
            wsem, xsem, xsend, xrecv, qsend, qrecv, ssend, srecv, fsend, frecv, osem, ysend, yrecv):
    me = lax.axis_index("sp")
    chip, core = me // 2, me % 2
    cx, cy, cz = chip // 4, (chip // 2) % 2, chip % 2
    partner = {"sp": chip * 2 + (1 - core)}
    mine = core * CHIPS + chip

    def peer(s):
        return ((cx + s // 4) % 2) * 4 + ((cy + (s // 2) % 2) % 2) * 2 + (cz + s % 2) % 2

    def on(d):
        return {"sp": d * 2 + core}

    weights = (wq_ref, wk_ref, wv_ref)

    def fetch_in(m, which):
        j = m * 3 + which
        at = core * HALF + peer(7 - m % 8) * 768 + (m // 8) * W
        return pltpu.make_async_copy(weights[which].at[:, :, pl.ds(pl.multiple_of(at, W), W)], ring.at[j % SLOTS], wsem.at[j % SLOTS, 0])

    def fetch_out(jc):
        slot, t, nb = jc % SLOTS, jc // 8, jc % 8
        at = core * HALF + nb * 768
        return [pltpu.make_async_copy(wo_ref.at[:, t, :, pl.ds(pl.multiple_of(at + i * W, W), W)], ring.at[slot, pl.ds(i * 16, 16)], wsem.at[slot, i])
                for i in range(3)]

    for which in range(3):
        fetch_in(0, which).start()

    def x_in(rows, cols, to, k):
        return pltpu.make_async_copy(x_ref.at[:, cols], to.at[rows, :], xsem.at[k])

    own = pl.ds(pl.multiple_of(core * 128, 128), 128)
    other = pl.ds(pl.multiple_of((1 - core) * 128, 128), 128)
    my_cols = pl.ds(pl.multiple_of(core * HALF, 128), HALF)
    other_cols = pl.ds(pl.multiple_of((1 - core) * HALF, 128), HALF)
    x_a, x_r = x_in(own, pl.ds(0, D), a_s, 0), x_in(own, my_cols, xres, 1)
    x_a.start()
    x_r.start()

    barrier = pltpu.get_barrier_semaphore()
    pl.semaphore_signal(barrier, inc=1, device_id=partner, device_id_type=pl.DeviceIdType.MESH)
    for s in range(1, 8):
        pl.semaphore_signal(barrier, inc=1, device_id=on(peer(s)), device_id_type=pl.DeviceIdType.MESH)
    pl.semaphore_wait(barrier, 8)

    def remote(src, dst, send, recv, device):
        return pltpu.make_async_remote_copy(src_ref=src, dst_ref=dst, send_sem=send, recv_sem=recv, device_id=device,
                                            device_id_type=pl.DeviceIdType.MESH)

    x_out = remote(x_ref, a_s.at[own, :], xsend.at[0], xrecv.at[0], partner)
    r_out = remote(x_ref.at[:, other_cols], xres.at[own, :], xsend.at[1], xrecv.at[1], partner)
    x_out.start()
    r_out.start()

    def norm(first):
        def rows16(r, c):
            rows = pl.ds(pl.multiple_of(first + r * 16, 16), 16)
            total = jnp.zeros((16, 512), jnp.float32)
            for n in range(0, D, 512):
                wide = a_s[rows, n : n + 512].astype(jnp.float32)
                total = total + wide * wide
            scale = lax.rsqrt(jnp.sum(total, axis=1, keepdims=True) * (1 / D) + 1e-6)
            for n in range(0, D, 512):
                wide = a_s[rows, n : n + 512].astype(jnp.float32)
                a_s[rows, n : n + 512] = (wide * scale * gain_ref[:, n : n + 512].astype(jnp.float32)).astype(jnp.bfloat16)
            return c

        lax.fori_loop(0, 8, rows16, 0)

    x_a.wait()
    norm(core * 128)
    x_out.wait_recv()
    norm((1 - core) * 128)

    def qkv_send(m, which):
        t, u = m // 8, m % 8
        return remote(stage.at[u * 3 + which], qkv.at[t, which, pl.ds(pl.multiple_of(chip * TOK, TOK), TOK), :],
                      qsend.at[u * 3 + which], qrecv.at[t * 3 + which, chip], on(peer(7 - u)))

    def qkv_arrived(t, which, s):
        d = peer(s)
        return remote(stage.at[0], qkv.at[t, which, pl.ds(pl.multiple_of(d * TOK, TOK), TOK), :], qsend.at[0], qrecv.at[t * 3 + which, d], on(d))

    def seen_send(t, s):
        d = peer(s)
        return remote(qkv.at[t, 0, pl.ds(pl.multiple_of(d * TOK, TOK), TOK), :], seen.at[t, mine], ssend.at[t, d], srecv.at[t, chip], on(d))

    def seen_arrived(t, s):
        d = peer(s)
        return remote(qkv.at[t, 0, pl.ds(0, TOK), :], seen.at[t, core * CHIPS + d], ssend.at[t, d], srecv.at[t, d], on(d))

    def forward(t, d):
        return remote(seen.at[t, core * CHIPS + d], seen.at[t, core * CHIPS + d], fsend.at[t, d], frecv.at[t, d], partner)

    def forward_arrived(t, d):
        g = (1 - core) * CHIPS + d
        return remote(seen.at[t, g], seen.at[t, g], fsend.at[t, d], frecv.at[t, d], partner)

    def attend(t, u):
        i = peer(7 - u)
        rows = pl.ds(pl.multiple_of(i * TOK, TOK), TOK)
        e = HEAD**-0.5 * LOG2E
        heads = [slice(h * HEAD, (h + 1) * HEAD) for h in range(2)]

        @pl.when(u == 0)
        def _():
            def arrived(s, c):
                for which in range(3):
                    qkv_arrived(t, which, s).wait_recv()
                return c

            lax.fori_loop(1, 8, arrived, 0)

        for h in range(2):
            top_s[h] = jnp.full((1, TOK), NEG, jnp.float32)
            mix_s[h] = jnp.zeros((HEAD + 8, TOK), jnp.float32)
        ones = jnp.ones((8, KB), jnp.bfloat16)

        def block(j, masked):
            here = pl.ds(pl.multiple_of(j * KB, KB), KB)
            scores = [_dot(qkv[t, 1, here, h], qkv[t, 0, rows, h], 1, 1) for h in heads]
            weights_, keeps = [], []
            if masked:
                gap = lax.broadcasted_iota(jnp.int32, (KB, TOK), 1) - lax.broadcasted_iota(jnp.int32, (KB, TOK), 0)
                ok = gap >= j * KB - i * TOK
            for h, s in enumerate(scores):
                if masked:
                    s = jnp.where(ok, s, HIDDEN)
                old = top_s[h]
                top = jnp.maximum(old, s.max(axis=0, keepdims=True))
                top_s[h] = top
                weights_.append(jnp.exp2((s - top) * e).astype(jnp.bfloat16))
                keeps.append(jnp.exp2((old - top) * e))
            for h, (p, keep) in enumerate(zip(weights_, keeps)):
                values = jnp.concatenate([qkv[t, 2, here, heads[h]].T, ones], axis=0)
                mix_s[h] = mix_s[h] * keep + _dot(values, p, 1, 0)

        def whole(j, c):
            block(j, False)
            return c

        lax.fori_loop(0, i // 2, whole, 0)
        block(i // 2, True)
        for h in range(2):
            total = mix_s[h, HEAD : HEAD + 1, :]
            qkv[t, 0, rows, heads[h]] = (mix_s[h, :HEAD, :] * (1 / total)).T.astype(jnp.bfloat16)

        @pl.when(u < 7)
        def _():
            seen_send(t, 7 - u).start()

        @pl.when(u == 7)
        def _():
            seen[t, mine] = qkv[t, 0, rows, :]

    def hand_on(t, u):
        @pl.when(u < 7)
        def _():
            seen_arrived(t, 7 - u).wait_recv()

        forward(t, peer(7 - u)).start()

    def chunk(m, c):
        t, u = m // 8, m % 8
        for which in range(3):
            j = m * 3 + which
            slot = j % SLOTS
            fetch_in(m, which).wait()

            @pl.when(m < 23)
            def _():
                fetch_in(m + 1, which).start()

            @pl.when(m == 23)
            def _():
                for f in fetch_out(which):
                    f.start()

            r = jnp.dot(a_s[...], ring[slot].reshape(D, W), preferred_element_type=jnp.float32).astype(jnp.bfloat16)
            if which < 2:
                wide = r.astype(jnp.float32)
                halves = []
                for h in range(2):
                    part = wide[:, h * HEAD : (h + 1) * HEAD]
                    halves.append((part * cos_ref[...] + pltpu.roll(part, HEAD // 2, 1) * sin_ref[...]).astype(jnp.bfloat16))
                r = jnp.concatenate(halves, axis=1)

            @pl.when((u < 7) & (t > 0))
            def _():
                qkv_send(m - 8, which).wait_send()

            @pl.when(u < 7)
            def _():
                stage[u * 3 + which] = r
                qkv_send(m, which).start()

            @pl.when(u == 7)
            def _():
                qkv[t, which, pl.ds(pl.multiple_of(chip * TOK, TOK), TOK), :] = r

        @pl.when(t > 0)
        def _():
            attend(t - 1, u)

        @pl.when(t > 1)
        def _():
            hand_on(t - 2, u)

        return c

    lax.fori_loop(0, 8 * PASSES, chunk, 0)

    x_r.wait()
    r_out.wait_recv()

    def all_here(t):
        def arrived(d, c):
            forward_arrived(t, d).wait_recv()
            return c

        lax.fori_loop(0, CHIPS, arrived, 0)

    def put(n):
        cols = pl.ds(pl.multiple_of(core * HALF + n * W, W), W)
        return (pltpu.make_async_copy(stage.at[n, own, :], y_ref.at[:, cols], osem.at[n]),
                remote(stage.at[n, other, :], y_ref.at[:, cols], ysend.at[n], yrecv.at[n], partner))

    def taken(n):
        cols = pl.ds(pl.multiple_of((1 - core) * HALF + n * W, W), W)
        return remote(stage.at[n, other, :], y_ref.at[:, cols], ysend.at[n], yrecv.at[n], partner)

    for t in range(PASSES):
        all_here(t)

        def out_block(nb, c, t=t):
            jc = t * 8 + nb
            slot = jc % SLOTS
            for f in fetch_out(jc):
                f.wait()

            @pl.when(jc + 3 < 24)
            def _():
                for f in fetch_out(jc + 3):
                    f.start()

            lhs = jnp.concatenate([seen[t, g] for g in range(16)], axis=1)
            for i in range(3):
                n = nb * 3 + i
                r = jnp.dot(lhs, ring[slot, i * 16 : (i + 1) * 16].reshape(D // 3, W), preferred_element_type=jnp.float32)
                if t == 0:
                    yacc[n] = r
                elif t == 1:
                    yacc[n] += r
                else:
                    x = xres[:, pl.ds(pl.multiple_of(n * W, W), W)].astype(jnp.float32)
                    stage[n] = (x + (yacc[n] + r)).astype(jnp.bfloat16)
                    for f in put(n):
                        f.start()
            if t == 0:
                attend(2, nb)
            if t < 2:
                hand_on(t + 1, nb)
            return c

        lax.fori_loop(0, 8, out_block, 0)
        if t == 0:
            def sent(n, c):
                for which in range(3):
                    qkv_send(16 + n, which).wait_send()
                return c

            lax.fori_loop(0, 7, sent, 0)

    x_out.wait_send()
    r_out.wait_send()
    for t in range(PASSES):
        def done(s, c, t=t):
            seen_send(t, s).wait_send()
            return c

        lax.fori_loop(1, 8, done, 0)

        def passed(d, c, t=t):
            forward(t, d).wait_send()
            return c

        lax.fori_loop(0, CHIPS, passed, 0)

    def last(n, c):
        keep, give = put(n)
        keep.wait()
        give.wait_send()
        taken(n).wait_recv()
        return c

    lax.fori_loop(0, 24, last, 0)


def solution(mesh):
    def step(x, gain, wq, wk, wv, wo):
        chip = lax.axis_index("sp") // 2
        place = chip * TOK + jnp.arange(TOK)
        half = HEAD // 2
        angle = place.astype(jnp.float32)[:, None] * THETA ** (-jnp.arange(half, dtype=jnp.float32) / half)
        cos, sin = jnp.cos(angle), jnp.sin(angle)
        cos, sin = jnp.concatenate([cos, cos], 1), jnp.concatenate([-sin, sin], 1)
        bf, f32 = jnp.bfloat16, jnp.float32
        dma, vmem, hbm = pltpu.SemaphoreType.DMA, pl.BlockSpec(memory_space=pltpu.VMEM), pl.BlockSpec(memory_space=pl.ANY)
        return pl.pallas_call(
            _kernel,
            out_shape=jax.ShapeDtypeStruct(x.shape, bf),
            in_specs=[hbm, vmem, vmem, vmem, hbm, hbm, hbm, hbm],
            out_specs=hbm,
            scratch_shapes=[
                pltpu.VMEM((TOK, D), bf),
                pltpu.VMEM((TOK, HALF), bf),
                pltpu.VMEM((SLOTS, 48, W, W), bf),
                pltpu.VMEM((PASSES, 3, 2048, W), bf),
                pltpu.VMEM((24, TOK, W), bf),
                pltpu.VMEM((PASSES, 16, TOK, W), bf),
                pltpu.VMEM((24, TOK, W), f32),
                pltpu.VMEM((2, 1, TOK), f32),
                pltpu.VMEM((2, HEAD + 8, TOK), f32),
                dma((SLOTS, 3)), dma((2,)), dma((2,)), dma((2,)), dma((24,)), dma((9, CHIPS)), dma((PASSES, CHIPS)), dma((PASSES, CHIPS)),
                dma((PASSES, CHIPS)), dma((PASSES, CHIPS)), dma((24,)), dma((24,)), dma((24,)),
            ],
            compiler_params=pltpu.CompilerParams(collective_id=0, has_side_effects=True, vmem_limit_bytes=67043328),
            name="layer",
        )(x, gain.reshape(1, D), cos, sin, *(w.reshape(48, W, D) for w in (wq, wk, wv)), wo.reshape(16, 3, W, D))

    tokens, whole = P(("dp", "sp"), None), P(None, None)
    return jax.shard_map(
        step,
        mesh=mesh,
        in_specs=(tokens, P(None), whole, whole, whole, whole),
        out_specs=tokens,
        check_vma=False,
    )
```

```python
import functools

import jax
import jax.numpy as jnp
from jax import lax
from jax.experimental import pallas as pl
from jax.experimental.pallas import tpu as pltpu
from jax.sharding import PartitionSpec as P

HEAD = 128
THETA = 10000
HIDDEN = -1e30
LOG2E = 1.4426950408889634
D = 12288
HALF = D // 2
CHIPS = 8
TOK = 256
W = 256
PASSES = 3
SLOTS = 4
KB = 512


def _dot(a, b, ca, cb):
    return lax.dot_general(a, b, (((ca,), (cb,)), ((), ())), preferred_element_type=jnp.float32)


def _kernel(x_ref, gain_ref, cos_ref, sin_ref, wq_ref, wk_ref, wv_ref, wo_ref, y_ref,
            a_s, xres, ring, qkv, tmp, stage, seen, yacc,
            wsem, xsem, xsend, xrecv, qsend, qrecv, ssend, srecv, fsend, frecv, osem, ysend, yrecv):
    me = lax.axis_index("sp")
    chip, core = me // 2, me % 2
    cx, cy, cz = chip // 4, (chip // 2) % 2, chip % 2
    partner = {"sp": chip * 2 + (1 - core)}
    mine = core * CHIPS + chip

    def peer(s):
        return ((cx + s // 4) % 2) * 4 + ((cy + (s // 2) % 2) % 2) * 2 + (cz + s % 2) % 2

    def on(d):
        return {"sp": d * 2 + core}

    weights = (wq_ref, wk_ref, wv_ref)

    def fetch_in(j, which):
        m = j // 3
        at = core * HALF + peer(7 - m % 8) * 768 + (m // 8) * W
        return pltpu.make_async_copy(weights[which].at[:, :, pl.ds(pl.multiple_of(at, W), W)], ring.at[j % SLOTS], wsem.at[j % SLOTS, 0])

    def fetch_out(jc):
        slot, t, nb = jc % SLOTS, jc // 8, jc % 8
        at = core * HALF + nb * 768
        return [pltpu.make_async_copy(wo_ref.at[:, t, :, pl.ds(pl.multiple_of(at + i * W, W), W)], ring.at[slot, pl.ds(i * 16, 16)], wsem.at[slot, i])
                for i in range(3)]

    def x_in(rows, cols, to, k):
        return pltpu.make_async_copy(x_ref.at[:, cols], to.at[rows, :], xsem.at[k])

    own = pl.ds(pl.multiple_of(core * 128, 128), 128)
    other = pl.ds(pl.multiple_of((1 - core) * 128, 128), 128)
    my_cols = pl.ds(pl.multiple_of(core * HALF, 128), HALF)
    other_cols = pl.ds(pl.multiple_of((1 - core) * HALF, 128), HALF)
    x_a, x_r = x_in(own, pl.ds(0, D), a_s, 0), x_in(own, my_cols, xres, 1)
    x_a.start()
    for which in range(3):
        fetch_in(which, which).start()
    x_r.start()

    barrier = pltpu.get_barrier_semaphore()
    pl.semaphore_signal(barrier, inc=1, device_id=partner, device_id_type=pl.DeviceIdType.MESH)
    for s in range(1, 8):
        pl.semaphore_signal(barrier, inc=1, device_id=on(peer(s)), device_id_type=pl.DeviceIdType.MESH)
    pl.semaphore_wait(barrier, 8)

    def remote(src, dst, send, recv, device):
        return pltpu.make_async_remote_copy(src_ref=src, dst_ref=dst, send_sem=send, recv_sem=recv, device_id=device,
                                            device_id_type=pl.DeviceIdType.MESH)

    x_out = remote(x_ref, a_s.at[own, :], xsend.at[0], xrecv.at[0], partner)
    r_out = remote(x_ref.at[:, other_cols], xres.at[own, :], xsend.at[1], xrecv.at[1], partner)
    x_out.start()
    r_out.start()

    def norm(first):
        def rows16(r, c):
            rows = pl.ds(pl.multiple_of(first + r * 16, 16), 16)
            total = jnp.zeros((16, 512), jnp.float32)
            for n in range(0, D, 512):
                wide = a_s[rows, n : n + 512].astype(jnp.float32)
                total = total + wide * wide
            scale = lax.rsqrt(jnp.sum(total, axis=1, keepdims=True) * (1 / D) + 1e-6)
            for n in range(0, D, 128):
                wide = a_s[rows, n : n + 128].astype(jnp.float32)
                gain = gain_ref[n // 128 : n // 128 + 1, :].astype(jnp.float32)
                a_s[rows, n : n + 128] = (wide * scale * gain).astype(jnp.bfloat16)
            return c

        lax.fori_loop(0, 8, rows16, 0)

    x_a.wait()
    norm(core * 128)
    x_out.wait_recv()
    norm((1 - core) * 128)

    def qkv_send(j):
        t, u, which = j // 24, (j // 3) % 8, j % 3
        return remote(stage.at[j % 24], qkv.at[t, which, chip], qsend.at[j % 24], qrecv.at[t * 3 + which, chip], on(peer(7 - u)))

    def qkv_arrived(t, which, s):
        d = peer(s)
        return remote(stage.at[0], qkv.at[t, which, d], qsend.at[0], qrecv.at[t * 3 + which, d], on(d))

    def seen_send(t, s):
        d = peer(s)
        return remote(qkv.at[t, 0, d], seen.at[t, mine], ssend.at[t, d], srecv.at[t, chip], on(d))

    def seen_arrived(t, s):
        d = peer(s)
        return remote(qkv.at[t, 0, 0], seen.at[t, core * CHIPS + d], ssend.at[t, d], srecv.at[t, d], on(d))

    def forward(t, d):
        return remote(seen.at[t, core * CHIPS + d], seen.at[t, core * CHIPS + d], fsend.at[t, d], frecv.at[t, d], partner)

    def forward_arrived(t, d):
        g = (1 - core) * CHIPS + d
        return remote(seen.at[t, g], seen.at[t, g], fsend.at[t, d], frecv.at[t, d], partner)

    def attend(t, u):
        i = peer(7 - u)
        e = HEAD**-0.5 * LOG2E
        heads = [slice(h * HEAD, (h + 1) * HEAD) for h in range(2)]

        @pl.when(u == 0)
        def _():
            def arrived(s, c):
                for which in range(3):
                    qkv_arrived(t, which, s).wait_recv()
                return c

            lax.fori_loop(1, 8, arrived, 0)

        def rounds(n):
            ones = jnp.ones((8, KB), jnp.bfloat16)
            gap = lax.broadcasted_iota(jnp.int32, (KB, TOK), 1) - lax.broadcasted_iota(jnp.int32, (KB, TOK), 0)

            def scores(j):
                return [_dot(qkv[t, 1, 2 * j : 2 * j + 2, :, h].reshape(KB, HEAD), qkv[t, 0, i, :, h], 1, 1) for h in heads]

            later, tops, mixes = scores(0), [None, None], [None, None]
            for j in range(n):
                now = later
                if j + 1 < n:
                    later = scores(j + 1)
                for h, s in enumerate(now):
                    if j == n - 1:
                        s = jnp.where(gap >= j * KB - i * TOK, s, HIDDEN)
                    top = s.max(axis=0, keepdims=True)
                    if j:
                        top = jnp.maximum(top, tops[h])
                    p = jnp.exp2((s - top) * e).astype(jnp.bfloat16)
                    values = jnp.concatenate([qkv[t, 2, 2 * j, heads[h], :], qkv[t, 2, 2 * j + 1, heads[h], :]], axis=1)
                    mix = _dot(jnp.concatenate([values, ones], axis=0), p, 1, 0)
                    mixes[h] = mixes[h] * jnp.exp2((tops[h] - top) * e) + mix if j else mix
                    tops[h] = top
            for h in range(2):
                qkv[t, 0, i, :, heads[h]] = (mixes[h][:HEAD] * (1 / mixes[h][HEAD : HEAD + 1])).T.astype(jnp.bfloat16)

        for n in range(1, 5):

            @pl.when(i // 2 == n - 1)
            def _():
                rounds(n)

        @pl.when(u < 7)
        def _():
            seen_send(t, 7 - u).start()

        @pl.when(u == 7)
        def _():
            seen[t, mine] = qkv[t, 0, i]

    def hand_on(t, u):
        @pl.when(u < 7)
        def _():
            seen_arrived(t, 7 - u).wait_recv()

        forward(t, peer(7 - u)).start()

    def ready(j):
        @pl.when((j >= 24) & ((j // 3) % 8 < 7))
        def _():
            qkv_send(j - 24).wait_send()

        @pl.when(j % 3 == 2)
        def _():
            stage[j % 24] = tmp[...].T

    def go(j):
        @pl.when((j // 3) % 8 < 7)
        def _():
            qkv_send(j).start()

        @pl.when((j // 3) % 8 == 7)
        def _():
            qkv[j // 24, j % 3, chip] = stage[j % 24]

    tmp[...] = jnp.zeros((TOK, W), jnp.bfloat16)

    def block(j, c):
        slot, t, u = j % SLOTS, j // 24, (j // 3) % 8
        fetch_in(j, 0).wait()

        for which in range(3):
            @pl.when((j < 69) & (j % 3 == which))
            def _():
                fetch_in(j + 3, which).start()

            @pl.when(j == 69 + which)
            def _():
                for f in fetch_out(which):
                    f.start()

        @pl.when(j > 0)
        def _():
            ready(j - 1)

        at = jnp.where(j % 3 == 0, 24, (j + 23) % 24)
        for h in range(2):
            cols = slice(h * HEAD, (h + 1) * HEAD)
            part = tmp[:, cols].astype(jnp.float32)
            stage[at, :, cols] = (part * cos_ref[...] + pltpu.roll(part, HEAD // 2, 1) * sin_ref[...]).astype(jnp.bfloat16)
        tmp[...] = jnp.dot(a_s[...], ring[slot].reshape(D, W), preferred_element_type=jnp.float32).astype(jnp.bfloat16)

        @pl.when(j > 0)
        def _():
            go(j - 1)

        @pl.when((t > 0) & (j % 3 == 2))
        def _():
            attend(t - 1, u)

        @pl.when((t > 1) & (j % 3 == 2))
        def _():
            hand_on(t - 2, u)

        return c

    lax.fori_loop(0, 24 * PASSES, block, 0)
    ready(71)
    go(71)

    x_r.wait()
    r_out.wait_recv()

    def all_here(t):
        def arrived(d, c):
            forward_arrived(t, d).wait_recv()
            return c

        lax.fori_loop(0, CHIPS, arrived, 0)

    def put(n):
        cols = pl.ds(pl.multiple_of(core * HALF + n * W, W), W)
        return (pltpu.make_async_copy(stage.at[n, own, :], y_ref.at[:, cols], osem.at[n]),
                remote(stage.at[n, other, :], y_ref.at[:, cols], ysend.at[n], yrecv.at[n], partner))

    def taken(n):
        cols = pl.ds(pl.multiple_of((1 - core) * HALF + n * W, W), W)
        return remote(stage.at[n, other, :], y_ref.at[:, cols], ysend.at[n], yrecv.at[n], partner)

    for t in range(PASSES):
        all_here(t)

        def out_block(nb, c, t=t):
            jc = t * 8 + nb
            slot = jc % SLOTS
            for f in fetch_out(jc):
                f.wait()

            @pl.when(jc + 3 < 24)
            def _():
                for f in fetch_out(jc + 3):
                    f.start()

            lhs = jnp.concatenate([seen[t, g] for g in range(16)], axis=1)
            for i in range(3):
                n = nb * 3 + i
                r = jnp.dot(lhs, ring[slot, i * 16 : (i + 1) * 16].reshape(D // 3, W), preferred_element_type=jnp.float32)
                if t == 0:
                    yacc[n] = r
                elif t == 1:
                    yacc[n] += r
                else:
                    x = xres[:, pl.ds(pl.multiple_of(n * W, W), W)].astype(jnp.float32)
                    stage[n] = (x + (yacc[n] + r)).astype(jnp.bfloat16)
            if t == 2:
                for i in range(3):
                    for f in put(nb * 3 + i):
                        f.start()
            if t == 0:
                attend(2, nb)
            if t < 2:
                hand_on(t + 1, nb)
            return c

        lax.fori_loop(0, 8, out_block, 0)
        if t == 0:
            def sent(n, c):
                qkv_send(48 + n).wait_send()
                return c

            lax.fori_loop(0, 21, sent, 0)

    x_out.wait_send()
    r_out.wait_send()
    for t in range(PASSES):
        def done(s, c, t=t):
            seen_send(t, s).wait_send()
            return c

        lax.fori_loop(1, 8, done, 0)

        def passed(d, c, t=t):
            forward(t, d).wait_send()
            return c

        lax.fori_loop(0, CHIPS, passed, 0)

    def last(n, c):
        keep, give = put(n)
        keep.wait()
        give.wait_send()
        taken(n).wait_recv()
        return c

    lax.fori_loop(0, 24, last, 0)


def solution(mesh):
    def step(x, gain, wq, wk, wv, wo):
        chip = lax.axis_index("sp") // 2
        place = chip * TOK + jnp.arange(TOK)
        half = HEAD // 2
        angle = place.astype(jnp.float32)[:, None] * THETA ** (-jnp.arange(half, dtype=jnp.float32) / half)
        cos, sin = jnp.cos(angle), jnp.sin(angle)
        cos, sin = jnp.concatenate([cos, cos], 1), jnp.concatenate([-sin, sin], 1)
        bf, f32 = jnp.bfloat16, jnp.float32
        dma, vmem, hbm = pltpu.SemaphoreType.DMA, pl.BlockSpec(memory_space=pltpu.VMEM), pl.BlockSpec(memory_space=pl.ANY)
        return pl.pallas_call(
            _kernel,
            out_shape=jax.ShapeDtypeStruct(x.shape, bf),
            in_specs=[hbm, vmem, vmem, vmem, hbm, hbm, hbm, hbm],
            out_specs=hbm,
            scratch_shapes=[
                pltpu.VMEM((TOK, D), bf),
                pltpu.VMEM((TOK, HALF), bf),
                pltpu.VMEM((SLOTS, 48, W, W), bf),
                pltpu.VMEM((PASSES, 3, CHIPS, TOK, W), bf),
                pltpu.VMEM((TOK, W), bf),
                pltpu.VMEM((25, TOK, W), bf),
                pltpu.VMEM((PASSES, 16, TOK, W), bf),
                pltpu.VMEM((24, TOK, W), f32),
                dma((SLOTS, 3)), dma((2,)), dma((2,)), dma((2,)), dma((24,)), dma((9, CHIPS)), dma((PASSES, CHIPS)), dma((PASSES, CHIPS)),
                dma((PASSES, CHIPS)), dma((PASSES, CHIPS)), dma((24,)), dma((24,)), dma((24,)),
            ],
            compiler_params=pltpu.CompilerParams(collective_id=0, has_side_effects=True, vmem_limit_bytes=67043328),
            name="layer",
        )(x, gain.reshape(D // 128, 128), cos, sin, *(w.reshape(48, W, D) for w in (wq, wk, wv)), wo.reshape(16, 3, W, D))

    tokens, whole = P(("dp", "sp"), None), P(None, None)
    return jax.shard_map(
        step,
        mesh=mesh,
        in_specs=(tokens, P(None), whole, whole, whole, whole),
        out_specs=tokens,
        check_vma=False,
    )
```

```python
import functools

import jax
import jax.numpy as jnp
from jax import lax
from jax.experimental import pallas as pl
from jax.experimental.pallas import tpu as pltpu
from jax.sharding import PartitionSpec as P

HEAD = 128
THETA = 10000
HIDDEN = -1e30
LOG2E = 1.4426950408889634
D = 12288
HALF = D // 2
CHIPS = 8
TOK = 256
W = 256
PASSES = 3
SLOTS = 5
KB = 512


def _dot(a, b, ca, cb):
    return lax.dot_general(a, b, (((ca,), (cb,)), ((), ())), preferred_element_type=jnp.float32)


def _kernel(x_ref, gain_ref, cos_ref, sin_ref, wq_ref, wk_ref, wv_ref, wo_ref, y_ref, xp_ref,
            a_s, ring, qkv, tmp, stage, seen, yacc, top_s, mix_s,
            wsem, xsem, xsend, xrecv, qsend, qrecv, ssend, srecv, fsend, frecv, osem, ysend, yrecv, xtsem):
    me = lax.axis_index("sp")
    div, rem = lax.div, lax.rem
    chip, core = div(me, 2), rem(me, 2)
    cx, cy, cz = div(chip, 4), rem(div(chip, 2), 2), rem(chip, 2)
    partner = {"sp": chip * 2 + (1 - core)}
    mine = core * CHIPS + chip

    def peer(s):
        x, y, z = (s // 4, s // 2 % 2, s % 2) if isinstance(s, int) else (div(s, 4), rem(div(s, 2), 2), rem(s, 2))
        return (cx + x - 2 * cx * x) * 4 + (cy + y - 2 * cy * y) * 2 + (cz + z - 2 * cz * z)

    def on(d):
        return {"sp": d * 2 + core}

    weights = (wq_ref, wk_ref, wv_ref)

    def fetch_in(j, which):
        m = div(j, 3)
        at = core * HALF + peer(7 - rem(m, 8)) * 768 + div(m, 8) * W
        return pltpu.make_async_copy(weights[which].at[:, :, pl.ds(pl.multiple_of(at, W), W)], ring.at[rem(j, SLOTS)], wsem.at[rem(j, SLOTS), 0])

    def fetch_out(jc):
        slot, t, nb = rem(jc + 72, SLOTS), div(jc, 8), rem(jc, 8)
        at = core * HALF + nb * 768
        return [pltpu.make_async_copy(wo_ref.at[:, t, :, pl.ds(pl.multiple_of(at + i * W, W), W)], ring.at[slot, pl.ds(i * 16, 16)], wsem.at[slot, i])
                for i in range(3)]

    own = pl.ds(pl.multiple_of(core * 128, 128), 128)
    other = pl.ds(pl.multiple_of((1 - core) * 128, 128), 128)
    my_cols = pl.ds(pl.multiple_of(core * HALF, 128), HALF)
    other_cols = pl.ds(pl.multiple_of((1 - core) * HALF, 128), HALF)
    x_a = pltpu.make_async_copy(x_ref, a_s.at[own, :], xsem.at[0])
    x_a.start()
    for b in range(SLOTS):
        fetch_in(jnp.int32(b), b % 3).start()

    barrier = pltpu.get_barrier_semaphore()
    pl.semaphore_signal(barrier, inc=1, device_id=partner, device_id_type=pl.DeviceIdType.MESH)
    for s in range(1, 8):
        pl.semaphore_signal(barrier, inc=1, device_id=on(peer(s)), device_id_type=pl.DeviceIdType.MESH)
    pl.semaphore_wait(barrier, 8)

    def remote(src, dst, send, recv, device):
        return pltpu.make_async_remote_copy(src_ref=src, dst_ref=dst, send_sem=send, recv_sem=recv, device_id=device,
                                            device_id_type=pl.DeviceIdType.MESH)

    x_out = remote(x_ref, a_s.at[own, :], xsend.at[0], xrecv.at[0], partner)
    r_out = remote(x_ref.at[:, other_cols], xp_ref, xsend.at[1], xrecv.at[1], partner)
    x_out.start()
    r_out.start()

    def norm(first):
        def rows16(r, c):
            rows = pl.ds(pl.multiple_of(first + r * 16, 16), 16)
            total = jnp.zeros((16, 512), jnp.float32)
            for n in range(0, D, 512):
                wide = a_s[rows, n : n + 512].astype(jnp.float32)
                total = total + wide * wide
            scale = lax.rsqrt(jnp.sum(total, axis=1, keepdims=True) * (1 / D) + 1e-6)
            for n in range(0, D, 128):
                wide = a_s[rows, n : n + 128].astype(jnp.float32)
                gain = gain_ref[n // 128 : n // 128 + 1, :].astype(jnp.float32)
                a_s[rows, n : n + 128] = (wide * scale * gain).astype(jnp.bfloat16)
            return c

        lax.fori_loop(0, 8, rows16, 0)

    x_a.wait()
    norm(core * 128)
    x_out.wait_recv()
    norm((1 - core) * 128)

    def qkv_send(j):
        t, u, which = div(j, 24), rem(div(j, 3), 8), rem(j, 3)
        return remote(stage.at[rem(j, 24)], qkv.at[t, which, chip], qsend.at[rem(j, 24)], qrecv.at[t * 3 + which, chip], on(peer(7 - u)))

    def qkv_arrived(t, which, s):
        d = peer(s)
        return remote(stage.at[0], qkv.at[t, which, d], qsend.at[0], qrecv.at[t * 3 + which, d], on(d))

    def seen_send(t, s):
        d = peer(s)
        return remote(qkv.at[t, 0, d], seen.at[t, mine], ssend.at[t, d], srecv.at[t, chip], on(d))

    def seen_arrived(t, s):
        d = peer(s)
        return remote(qkv.at[t, 0, 0], seen.at[t, core * CHIPS + d], ssend.at[t, d], srecv.at[t, d], on(d))

    def forward(t, d):
        return remote(seen.at[t, core * CHIPS + d], seen.at[t, core * CHIPS + d], fsend.at[t, d], frecv.at[t, d], partner)

    def forward_arrived(t, d):
        g = (1 - core) * CHIPS + d
        return remote(seen.at[t, g], seen.at[t, g], fsend.at[t, d], frecv.at[t, d], partner)

    heads = [slice(h * HEAD, (h + 1) * HEAD) for h in range(2)]
    e = HEAD**-0.5 * LOG2E

    def all_arrived(t):
        def arrived(s, c):
            for which in range(3):
                qkv_arrived(t, which, s).wait_recv()
            return c

        lax.fori_loop(1, 8, arrived, 0)

    def deliver(t, u):
        @pl.when(u < 7)
        def _():
            seen_send(t, 7 - u).start()

        @pl.when(u == 7)
        def _():
            seen[t, mine] = qkv[t, 0, chip]

    def attend_step(t, u, kb):
        i, par = peer(7 - u), rem(u, 2)
        ones = jnp.ones((8, KB), jnp.bfloat16)
        gap = lax.broadcasted_iota(jnp.int32, (KB, TOK), 1) - lax.broadcasted_iota(jnp.int32, (KB, TOK), 0)
        ok = gap >= kb * KB - i * TOK
        scores = [_dot(qkv[t, 1, pl.ds(2 * kb, 2), :, h].reshape(KB, HEAD), qkv[t, 0, i, :, h], 1, 1) for h in heads]
        for h, s in enumerate(scores):
            s = jnp.where(ok, s, HIDDEN)
            old = top_s[par, h]
            top = jnp.maximum(old, s.max(axis=0, keepdims=True))
            top_s[par, h] = top
            p = jnp.exp2((s - top) * e).astype(jnp.bfloat16)
            values = jnp.concatenate([qkv[t, 2, 2 * kb, heads[h], :], qkv[t, 2, 2 * kb + 1, heads[h], :]], axis=1)
            mix_s[par, h] = mix_s[par, h] * jnp.exp2((old - top) * e) + _dot(jnp.concatenate([values, ones], axis=0), p, 1, 0)

    def attend_end(t, u):
        i, par = peer(7 - u), rem(u, 2)
        for h in range(2):
            qkv[t, 0, i, :, heads[h]] = (mix_s[par, h, :HEAD, :] * (1 / mix_s[par, h, HEAD : HEAD + 1, :])).T.astype(jnp.bfloat16)
            top_s[par, h] = jnp.full((1, TOK), HIDDEN, jnp.float32)
        deliver(t, u)

    def attend(t, u):
        i = peer(7 - u)

        @pl.when(u == 0)
        def _():
            all_arrived(t)

        def rounds(n):
            ones = jnp.ones((8, KB), jnp.bfloat16)
            gap = lax.broadcasted_iota(jnp.int32, (KB, TOK), 1) - lax.broadcasted_iota(jnp.int32, (KB, TOK), 0)

            def scores(j):
                return [_dot(qkv[t, 1, 2 * j : 2 * j + 2, :, h].reshape(KB, HEAD), qkv[t, 0, i, :, h], 1, 1) for h in heads]

            later, tops, mixes = scores(0), [None, None], [None, None]
            for j in range(n):
                now = later
                if j + 1 < n:
                    later = scores(j + 1)
                for h, s in enumerate(now):
                    if j == n - 1:
                        s = jnp.where(gap >= j * KB - i * TOK, s, HIDDEN)
                    top = s.max(axis=0, keepdims=True)
                    if j:
                        top = jnp.maximum(top, tops[h])
                    p = jnp.exp2((s - top) * e).astype(jnp.bfloat16)
                    values = jnp.concatenate([qkv[t, 2, 2 * j, heads[h], :], qkv[t, 2, 2 * j + 1, heads[h], :]], axis=1)
                    mix = _dot(jnp.concatenate([values, ones], axis=0), p, 1, 0)
                    mixes[h] = mixes[h] * jnp.exp2((tops[h] - top) * e) + mix if j else mix
                    tops[h] = top
            for h in range(2):
                qkv[t, 0, i, :, heads[h]] = (mixes[h][:HEAD] * (1 / mixes[h][HEAD : HEAD + 1])).T.astype(jnp.bfloat16)

        for n in range(1, 5):

            @pl.when(div(i, 2) == n - 1)
            def _():
                rounds(n)

        deliver(t, u)

    def hand_on(t, u):
        @pl.when(u < 7)
        def _():
            seen_arrived(t, 7 - u).wait_recv()

        forward(t, peer(7 - u)).start()

    def ready(j, n):
        @pl.when((j >= 24) & (rem(div(j, 3), 8) < 7))
        def _():
            qkv_send(j - 24).wait_send()

        @pl.when(rem(j, 3) == 2)
        def _():
            stage[rem(j, 24)] = tmp[n].T

    def go(j):
        @pl.when(rem(div(j, 3), 8) < 7)
        def _():
            qkv_send(j).start()

        @pl.when(rem(div(j, 3), 8) == 7)
        def _():
            qkv[div(j, 24), rem(j, 3), chip] = stage[rem(j, 24)]

    def turn(j, n):
        at = jnp.where(rem(j, 3) == 2, 24, rem(j, 24))
        for h in range(2):
            part = tmp[n, :, heads[h]].astype(jnp.float32)
            stage[at, :, heads[h]] = (part * cos_ref[...] + pltpu.roll(part, HEAD // 2, 1) * sin_ref[...]).astype(jnp.bfloat16)

    def project(j, n):
        tmp[n] = jnp.dot(a_s[...], ring[rem(j, SLOTS)].reshape(D, W), preferred_element_type=jnp.float32).astype(jnp.bfloat16)

    tmp[...] = jnp.zeros((2, TOK, W), jnp.bfloat16)
    mix_s[...] = jnp.zeros((2, 2, HEAD + 8, TOK), jnp.float32)
    top_s[...] = jnp.full((2, 2, 1, TOK), HIDDEN, jnp.float32)

    def pair(k, state):
        u, kb = state
        j, t, kk = 2 * k, div(k, 12), rem(k, 12)

        @pl.when(k > 0)
        def _():
            for b in (j + 3, j + 4):
                for which in range(3):

                    @pl.when((b < 72) & (rem(b, 3) == which))
                    def _():
                        fetch_in(b, which).start()

                @pl.when(b >= 72)
                def _():
                    for f in fetch_out(b - 72):
                        f.start()

            ready(j - 2, 0)
            ready(j - 1, 1)

        fetch_in(j, 0).wait()
        fetch_in(j + 1, 0).wait()

        busy = (t > 0) & (kk >= 2)
        u = jnp.where(kk == 2, 0, u)
        kb = jnp.where(kk == 2, 0, kb)
        end_a = kb == div(peer(7 - jnp.minimum(u, 7)), 2)
        u_b, kb_b = jnp.where(end_a, u + 1, u), jnp.where(end_a, 0, kb + 1)
        end_b = kb_b == div(peer(7 - jnp.minimum(u_b, 7)), 2)
        u_c, kb_c = jnp.where(end_b, u_b + 1, u_b), jnp.where(end_b, 0, kb_b + 1)
        before = jnp.maximum(j - 2, 0)

        @pl.when(busy & (kk == 2))
        def _():
            all_arrived(t - 1)

        @pl.when(jnp.logical_not(busy))
        def _():
            turn(before, 0)
            turn(before + 1, 1)
            project(j, 0)
            project(j + 1, 1)

        @pl.when(busy)
        def _():
            turn(before, 0)
            turn(before + 1, 1)
            project(j, 0)
            attend_step(t - 1, u, kb)
            project(j + 1, 1)
            attend_step(t - 1, u_b, kb_b)

        @pl.when(k > 0)
        def _():
            go(j - 2)
            go(j - 1)

        @pl.when(busy & end_a)
        def _():
            attend_end(t - 1, u)

        @pl.when(busy & end_b)
        def _():
            attend_end(t - 1, u_b)

        @pl.when((t == 2) & (kk >= 2) & (kk < 10))
        def _():
            hand_on(0, kk - 2)

        return jnp.where(busy, u_c, 0), jnp.where(busy, kb_c, 0)

    lax.fori_loop(0, 12 * PASSES, pair, (jnp.int32(0), jnp.int32(0)))
    for f in fetch_out(jnp.int32(3)):
        f.start()
    for n in range(2):
        ready(jnp.int32(70 + n), n)
        turn(jnp.int32(70 + n), n)
        go(jnp.int32(70 + n))

    def x_tile(n):
        half = core * HALF + n * W
        return (pltpu.make_async_copy(x_ref.at[:, pl.ds(pl.multiple_of(half, W), W)], stage.at[n, own, :], xtsem.at[n, 0]),
                pltpu.make_async_copy(xp_ref.at[:, pl.ds(pl.multiple_of(n * W, W), W)], stage.at[n, other, :], xtsem.at[n, 1]))

    def all_here(t):
        def arrived(d, c):
            forward_arrived(t, d).wait_recv()
            return c

        lax.fori_loop(0, CHIPS, arrived, 0)

    def put(n):
        cols = pl.ds(pl.multiple_of(core * HALF + n * W, W), W)
        return (pltpu.make_async_copy(stage.at[n, own, :], y_ref.at[:, cols], osem.at[n]),
                remote(stage.at[n, other, :], y_ref.at[:, cols], ysend.at[n], yrecv.at[n], partner))

    def taken(n):
        cols = pl.ds(pl.multiple_of((1 - core) * HALF + n * W, W), W)
        return remote(stage.at[n, other, :], y_ref.at[:, cols], ysend.at[n], yrecv.at[n], partner)

    for t in range(PASSES):
        all_here(t)

        def out_block(nb, c, t=t):
            jc = t * 8 + nb
            slot = rem(jc + 72, SLOTS)

            @pl.when(jc + 4 < 24)
            def _():
                for f in fetch_out(jc + 4):
                    f.start()

            for f in fetch_out(jc):
                f.wait()
            if t == 2:
                for i in range(3):
                    for f in x_tile(nb * 3 + i):
                        f.wait()

            lhs = jnp.concatenate([seen[t, g] for g in range(16)], axis=1)
            for i in range(3):
                n = nb * 3 + i
                r = jnp.dot(lhs, ring[slot, i * 16 : (i + 1) * 16].reshape(D // 3, W), preferred_element_type=jnp.float32)
                if t == 0:
                    yacc[n] = r
                elif t == 1:
                    yacc[n] += r
                else:
                    stage[n] = (stage[n].astype(jnp.float32) + (yacc[n] + r)).astype(jnp.bfloat16)
            if t == 2:
                for i in range(3):
                    for f in put(nb * 3 + i):
                        f.start()
            if t == 0:
                attend(2, nb)
            if t < 2:
                hand_on(t + 1, nb)
            return c

        lax.fori_loop(0, 8, out_block, 0)
        if t == 0:
            def sent(n, c):
                qkv_send(48 + n).wait_send()
                return c

            lax.fori_loop(0, 21, sent, 0)
            r_out.wait_recv()

            def back(n, c):
                for f in x_tile(n):
                    f.start()
                return c

            lax.fori_loop(0, 24, back, 0)

    x_out.wait_send()
    r_out.wait_send()
    for t in range(PASSES):
        def done(s, c, t=t):
            seen_send(t, s).wait_send()
            return c

        lax.fori_loop(1, 8, done, 0)

        def passed(d, c, t=t):
            forward(t, d).wait_send()
            return c

        lax.fori_loop(0, CHIPS, passed, 0)

    def last(n, c):
        keep, give = put(n)
        keep.wait()
        give.wait_send()
        taken(n).wait_recv()
        return c

    lax.fori_loop(0, 24, last, 0)


def solution(mesh):
    def step(x, gain, wq, wk, wv, wo):
        chip = lax.axis_index("sp") // 2
        place = chip * TOK + jnp.arange(TOK)
        half = HEAD // 2
        angle = place.astype(jnp.float32)[:, None] * THETA ** (-jnp.arange(half, dtype=jnp.float32) / half)
        cos, sin = jnp.cos(angle), jnp.sin(angle)
        cos, sin = jnp.concatenate([cos, cos], 1), jnp.concatenate([-sin, sin], 1)
        bf, f32 = jnp.bfloat16, jnp.float32
        dma, vmem, hbm = pltpu.SemaphoreType.DMA, pl.BlockSpec(memory_space=pltpu.VMEM), pl.BlockSpec(memory_space=pl.ANY)
        return pl.pallas_call(
            _kernel,
            out_shape=[jax.ShapeDtypeStruct(x.shape, bf), jax.ShapeDtypeStruct((x.shape[0], HALF), bf)],
            in_specs=[hbm, vmem, vmem, vmem, hbm, hbm, hbm, hbm],
            out_specs=[hbm, hbm],
            scratch_shapes=[
                pltpu.VMEM((TOK, D), bf),
                pltpu.VMEM((SLOTS, 48, W, W), bf),
                pltpu.VMEM((PASSES, 3, CHIPS, TOK, W), bf),
                pltpu.VMEM((2, TOK, W), bf),
                pltpu.VMEM((25, TOK, W), bf),
                pltpu.VMEM((PASSES, 16, TOK, W), bf),
                pltpu.VMEM((24, TOK, W), f32),
                pltpu.VMEM((2, 2, 1, TOK), f32),
                pltpu.VMEM((2, 2, HEAD + 8, TOK), f32),
                dma((SLOTS, 3)), dma((2,)), dma((2,)), dma((2,)), dma((24,)), dma((9, CHIPS)), dma((PASSES, CHIPS)), dma((PASSES, CHIPS)),
                dma((PASSES, CHIPS)), dma((PASSES, CHIPS)), dma((24,)), dma((24,)), dma((24,)), dma((24, 2)),
            ],
            compiler_params=pltpu.CompilerParams(collective_id=0, has_side_effects=True, vmem_limit_bytes=67043328),
            name="layer",
        )(x, gain.reshape(D // 128, 128), cos, sin, *(w.reshape(48, W, D) for w in (wq, wk, wv)), wo.reshape(16, 3, W, D))[0]

    tokens, whole = P(("dp", "sp"), None), P(None, None)
    return jax.shard_map(
        step,
        mesh=mesh,
        in_specs=(tokens, P(None), whole, whole, whole, whole),
        out_specs=tokens,
        check_vma=False,
    )
```

```python
import functools

import jax
import jax.numpy as jnp
from jax import lax
from jax.experimental import pallas as pl
from jax.experimental.pallas import tpu as pltpu
from jax.sharding import PartitionSpec as P

HEAD = 128
THETA = 10000
HIDDEN = -1e30
LOG2E = 1.4426950408889634
D = 12288
HALF = D // 2
CHIPS = 8
TOK = 256
W = 256
PASSES = 3
SLOTS = 5
KB = 512


def _dot(a, b, ca, cb):
    return lax.dot_general(a, b, (((ca,), (cb,)), ((), ())), preferred_element_type=jnp.float32)


def _kernel(x_ref, gain_ref, cos_ref, sin_ref, wq_ref, wk_ref, wv_ref, wo_ref, y_ref, xp_ref,
            a_s, ring, qkv, tmp, stage, seen, yacc, top_s, mix_s,
            wsem, xsem, xsend, xrecv, qsend, qrecv, ssend, srecv, fsend, frecv, osem, ysend, yrecv, xtsem):
    me = lax.axis_index("sp")
    div, rem = lax.div, lax.rem
    chip, core = div(me, 2), rem(me, 2)
    cx, cy, cz = div(chip, 4), rem(div(chip, 2), 2), rem(chip, 2)
    partner = {"sp": chip * 2 + (1 - core)}
    mine = core * CHIPS + chip

    def peer(s):
        x, y, z = (s // 4, s // 2 % 2, s % 2) if isinstance(s, int) else (div(s, 4), rem(div(s, 2), 2), rem(s, 2))
        return (cx + x - 2 * cx * x) * 4 + (cy + y - 2 * cy * y) * 2 + (cz + z - 2 * cz * z)

    def turn_of(u):
        half, odd = div(u, 2), rem(u, 2)
        return (1 - odd) * (7 - half) + odd * rem(half + 1, 4)

    def on(d):
        return {"sp": d * 2 + core}

    weights = (wq_ref, wk_ref, wv_ref)

    def fetch_in(j, which):
        m = div(j, 3)
        at = core * HALF + peer(turn_of(rem(m, 8))) * 768 + div(m, 8) * W
        return pltpu.make_async_copy(weights[which].at[:, :, pl.ds(pl.multiple_of(at, W), W)], ring.at[rem(j, SLOTS)], wsem.at[rem(j, SLOTS), 0])

    def fetch_out(jc):
        slot, t, nb = rem(jc + 72, SLOTS), div(jc, 8), rem(jc, 8)
        at = core * HALF + nb * 768
        return [pltpu.make_async_copy(wo_ref.at[:, t, :, pl.ds(pl.multiple_of(at + i * W, W), W)], ring.at[slot, pl.ds(i * 16, 16)], wsem.at[slot, i])
                for i in range(3)]

    own = pl.ds(pl.multiple_of(core * 128, 128), 128)
    other = pl.ds(pl.multiple_of((1 - core) * 128, 128), 128)
    other_cols = pl.ds(pl.multiple_of((1 - core) * HALF, 128), HALF)
    x_a = pltpu.make_async_copy(x_ref, a_s.at[own, :], xsem.at[0])
    x_a.start()
    for b in range(2):
        fetch_in(jnp.int32(b), b % 3).start()

    barrier = pltpu.get_barrier_semaphore()
    pl.semaphore_signal(barrier, inc=1, device_id=partner, device_id_type=pl.DeviceIdType.MESH)
    for s in range(1, 8):
        pl.semaphore_signal(barrier, inc=1, device_id=on(peer(s)), device_id_type=pl.DeviceIdType.MESH)
    pl.semaphore_wait(barrier, 8)

    def remote(src, dst, send, recv, device):
        return pltpu.make_async_remote_copy(src_ref=src, dst_ref=dst, send_sem=send, recv_sem=recv, device_id=device,
                                            device_id_type=pl.DeviceIdType.MESH)

    x_out = remote(x_ref, a_s.at[own, :], xsend.at[0], xrecv.at[0], partner)
    r_out = remote(x_ref.at[:, other_cols], xp_ref, xsend.at[1], xrecv.at[1], partner)
    x_out.start()
    for b in range(2, SLOTS):
        fetch_in(jnp.int32(b), b % 3).start()

    def norm(first):
        def rows16(r, c):
            rows = pl.ds(pl.multiple_of(first + r * 16, 16), 16)
            total = jnp.zeros((16, 512), jnp.float32)
            for n in range(0, D, 512):
                wide = a_s[rows, n : n + 512].astype(jnp.float32)
                total = total + wide * wide
            scale = lax.rsqrt(jnp.sum(total, axis=1, keepdims=True) * (1 / D) + 1e-6)
            for n in range(0, D, 128):
                wide = a_s[rows, n : n + 128].astype(jnp.float32)
                gain = gain_ref[n // 128 : n // 128 + 1, :].astype(jnp.float32)
                a_s[rows, n : n + 128] = (wide * scale * gain).astype(jnp.bfloat16)
            return c

        lax.fori_loop(0, 8, rows16, 0)

    x_a.wait()
    norm(core * 128)
    x_out.wait_recv()
    norm((1 - core) * 128)
    r_out.start()

    def qkv_send(j):
        t, u, which = div(j, 24), rem(div(j, 3), 8), rem(j, 3)
        return remote(stage.at[rem(j, 24)], qkv.at[t, which, chip], qsend.at[rem(j, 24)], qrecv.at[t * 3 + which, chip], on(peer(turn_of(u))))

    def qkv_arrived(t, which, s):
        d = peer(s)
        return remote(stage.at[0], qkv.at[t, which, d], qsend.at[0], qrecv.at[t * 3 + which, d], on(d))

    def seen_send(t, s):
        d = peer(s)
        return remote(qkv.at[t, 0, d], seen.at[t, mine], ssend.at[t, d], srecv.at[t, chip], on(d))

    def seen_arrived(t, s):
        d = peer(s)
        return remote(qkv.at[t, 0, 0], seen.at[t, core * CHIPS + d], ssend.at[t, d], srecv.at[t, d], on(d))

    def forward(t, d):
        return remote(seen.at[t, core * CHIPS + d], seen.at[t, core * CHIPS + d], fsend.at[t, d], frecv.at[t, d], partner)

    def forward_arrived(t, d):
        g = (1 - core) * CHIPS + d
        return remote(seen.at[t, g], seen.at[t, g], fsend.at[t, d], frecv.at[t, d], partner)

    heads = [slice(h * HEAD, (h + 1) * HEAD) for h in range(2)]
    e = HEAD**-0.5 * LOG2E

    def all_arrived(t):
        def arrived(s, c):
            for which in range(3):
                qkv_arrived(t, which, s).wait_recv()
            return c

        lax.fori_loop(1, 8, arrived, 0)

    def deliver(t, u):
        @pl.when(u < 7)
        def _():
            seen_send(t, turn_of(u)).start()

        @pl.when(u == 7)
        def _():
            seen[t, mine] = qkv[t, 0, chip]

    def attend_step(t, u, kb):
        i, par = peer(turn_of(u)), rem(u, 2)
        ones = jnp.ones((8, KB), jnp.bfloat16)
        gap = lax.broadcasted_iota(jnp.int32, (KB, TOK), 1) - lax.broadcasted_iota(jnp.int32, (KB, TOK), 0)
        ok = gap >= kb * KB - i * TOK
        scores = [_dot(qkv[t, 1, pl.ds(2 * kb, 2), :, h].reshape(KB, HEAD), qkv[t, 0, i, :, h], 1, 1) for h in heads]
        for h, s in enumerate(scores):
            s = jnp.where(ok, s, HIDDEN)
            old = top_s[par, h]
            top = jnp.maximum(old, s.max(axis=0, keepdims=True))
            top_s[par, h] = top
            p = jnp.exp2((s - top) * e).astype(jnp.bfloat16)
            values = jnp.concatenate([qkv[t, 2, 2 * kb, heads[h], :], qkv[t, 2, 2 * kb + 1, heads[h], :]], axis=1)
            mix_s[par, h] = mix_s[par, h] * jnp.exp2((old - top) * e) + _dot(jnp.concatenate([values, ones], axis=0), p, 1, 0)

    def attend_end(t, u):
        i, par = peer(turn_of(u)), rem(u, 2)
        for h in range(2):
            qkv[t, 0, i, :, heads[h]] = (mix_s[par, h, :HEAD, :] * (1 / mix_s[par, h, HEAD : HEAD + 1, :])).T.astype(jnp.bfloat16)
            top_s[par, h] = jnp.full((1, TOK), HIDDEN, jnp.float32)
        deliver(t, u)

    def attend(t, u):
        i = peer(turn_of(u))

        @pl.when(u == 0)
        def _():
            all_arrived(t)

        def rounds(n):
            ones = jnp.ones((8, KB), jnp.bfloat16)
            gap = lax.broadcasted_iota(jnp.int32, (KB, TOK), 1) - lax.broadcasted_iota(jnp.int32, (KB, TOK), 0)

            def scores(j):
                return [_dot(qkv[t, 1, 2 * j : 2 * j + 2, :, h].reshape(KB, HEAD), qkv[t, 0, i, :, h], 1, 1) for h in heads]

            later, tops, mixes = scores(0), [None, None], [None, None]
            for j in range(n):
                now = later
                if j + 1 < n:
                    later = scores(j + 1)
                for h, s in enumerate(now):
                    if j == n - 1:
                        s = jnp.where(gap >= j * KB - i * TOK, s, HIDDEN)
                    top = s.max(axis=0, keepdims=True)
                    if j:
                        top = jnp.maximum(top, tops[h])
                    p = jnp.exp2((s - top) * e).astype(jnp.bfloat16)
                    values = jnp.concatenate([qkv[t, 2, 2 * j, heads[h], :], qkv[t, 2, 2 * j + 1, heads[h], :]], axis=1)
                    mix = _dot(jnp.concatenate([values, ones], axis=0), p, 1, 0)
                    mixes[h] = mixes[h] * jnp.exp2((tops[h] - top) * e) + mix if j else mix
                    tops[h] = top
            for h in range(2):
                qkv[t, 0, i, :, heads[h]] = (mixes[h][:HEAD] * (1 / mixes[h][HEAD : HEAD + 1])).T.astype(jnp.bfloat16)

        for n in range(1, 5):

            @pl.when(div(i, 2) == n - 1)
            def _():
                rounds(n)

        deliver(t, u)

    def hand_on(t, u):
        @pl.when(u < 7)
        def _():
            seen_arrived(t, turn_of(u)).wait_recv()

        forward(t, peer(turn_of(u))).start()

    def ready(j, n):
        @pl.when((j >= 24) & (rem(div(j, 3), 8) < 7))
        def _():
            qkv_send(j - 24).wait_send()

    def go(j):
        @pl.when(rem(div(j, 3), 8) < 7)
        def _():
            qkv_send(j).start()

        @pl.when(rem(div(j, 3), 8) == 7)
        def _():
            qkv[div(j, 24), rem(j, 3), chip] = stage[rem(j, 24)]

    def turn(j, n):
        values, slot = rem(j, 3) == 2, rem(j, 24)
        at = jnp.where(values, 24, slot)
        stage[jnp.where(values, slot, 24)] = tmp[n].T
        for h in range(2):
            part = tmp[n, :, heads[h]].astype(jnp.float32)
            stage[at, :, heads[h]] = (part * cos_ref[...] + pltpu.roll(part, HEAD // 2, 1) * sin_ref[...]).astype(jnp.bfloat16)

    def project(j, n):
        tmp[n] = jnp.dot(a_s[...], ring[rem(j, SLOTS)].reshape(D, W), preferred_element_type=jnp.float32).astype(jnp.bfloat16)

    tmp[...] = jnp.zeros((2, TOK, W), jnp.bfloat16)
    mix_s[...] = jnp.zeros((2, 2, HEAD + 8, TOK), jnp.float32)
    top_s[...] = jnp.full((2, 2, 1, TOK), HIDDEN, jnp.float32)

    def pair(k, state):
        u, kb = state
        j, t, kk = 2 * k, div(k, 12), rem(k, 12)

        @pl.when(k > 0)
        def _():
            for b in (j + 3, j + 4):
                for which in range(3):

                    @pl.when((b < 72) & (rem(b, 3) == which))
                    def _():
                        fetch_in(b, which).start()

                @pl.when(b >= 72)
                def _():
                    for f in fetch_out(b - 72):
                        f.start()

            ready(j - 2, 0)
            ready(j - 1, 1)

        fetch_in(j, 0).wait()
        fetch_in(j + 1, 0).wait()

        busy = (t > 0) & (kk >= 2)
        u = jnp.where(kk == 2, 0, u)
        kb = jnp.where(kk == 2, 0, kb)
        end_a = kb == div(peer(turn_of(jnp.minimum(u, 7))), 2)
        u_b, kb_b = jnp.where(end_a, u + 1, u), jnp.where(end_a, 0, kb + 1)
        end_b = kb_b == div(peer(turn_of(jnp.minimum(u_b, 7))), 2)
        u_c, kb_c = jnp.where(end_b, u_b + 1, u_b), jnp.where(end_b, 0, kb_b + 1)
        before = jnp.maximum(j - 2, 0)

        @pl.when(busy & (kk == 2))
        def _():
            all_arrived(t - 1)

        @pl.when(jnp.logical_not(busy))
        def _():
            turn(before, 0)
            turn(before + 1, 1)
            project(j, 0)
            project(j + 1, 1)

        @pl.when(busy)
        def _():
            turn(before, 0)
            turn(before + 1, 1)
            project(j, 0)
            attend_step(t - 1, u, kb)
            project(j + 1, 1)
            attend_step(t - 1, u_b, kb_b)

        @pl.when(k > 0)
        def _():
            go(j - 2)
            go(j - 1)

        @pl.when(busy & end_a)
        def _():
            attend_end(t - 1, u)

        @pl.when(busy & end_b)
        def _():
            attend_end(t - 1, u_b)

        @pl.when((t == 2) & (kk >= 2) & (kk < 10))
        def _():
            hand_on(0, kk - 2)

        return jnp.where(busy, u_c, 0), jnp.where(busy, kb_c, 0)

    lax.fori_loop(0, 12 * PASSES, pair, (jnp.int32(0), jnp.int32(0)))
    for f in fetch_out(jnp.int32(3)):
        f.start()
    for n in range(2):
        ready(jnp.int32(70 + n), n)
        turn(jnp.int32(70 + n), n)
        go(jnp.int32(70 + n))

    def x_tile(n):
        half = core * HALF + n * W
        return (pltpu.make_async_copy(x_ref.at[:, pl.ds(pl.multiple_of(half, W), W)], stage.at[n, own, :], xtsem.at[n, 0]),
                pltpu.make_async_copy(xp_ref.at[:, pl.ds(pl.multiple_of(n * W, W), W)], stage.at[n, other, :], xtsem.at[n, 1]))

    def all_here(t):
        def arrived(d, c):
            forward_arrived(t, d).wait_recv()
            return c

        lax.fori_loop(0, CHIPS, arrived, 0)

    def put(n):
        cols = pl.ds(pl.multiple_of(core * HALF + n * W, W), W)
        return (pltpu.make_async_copy(stage.at[n, own, :], y_ref.at[:, cols], osem.at[n]),
                remote(stage.at[n, other, :], y_ref.at[:, cols], ysend.at[n], yrecv.at[n], partner))

    def taken(n):
        cols = pl.ds(pl.multiple_of((1 - core) * HALF + n * W, W), W)
        return remote(stage.at[n, other, :], y_ref.at[:, cols], ysend.at[n], yrecv.at[n], partner)

    for t in range(PASSES):
        all_here(t)

        def out_block(nb, c, t=t):
            jc = t * 8 + nb
            slot = rem(jc + 72, SLOTS)

            @pl.when(jc + 4 < 24)
            def _():
                for f in fetch_out(jc + 4):
                    f.start()

            for f in fetch_out(jc):
                f.wait()
            if t == 2:
                for i in range(3):
                    for f in x_tile(nb * 3 + i):
                        f.wait()

            lhs = jnp.concatenate([seen[t, g] for g in range(16)], axis=1)
            for i in range(3):
                n = nb * 3 + i
                r = jnp.dot(lhs, ring[slot, i * 16 : (i + 1) * 16].reshape(D // 3, W), preferred_element_type=jnp.float32)
                if t == 0:
                    yacc[n] = r
                elif t == 1:
                    yacc[n] += r
                else:
                    stage[n] = (stage[n].astype(jnp.float32) + (yacc[n] + r)).astype(jnp.bfloat16)
            if t == 2:
                for i in range(3):
                    for f in put(nb * 3 + i):
                        f.start()
            if t == 0:

                @pl.when(nb >= 4)
                def _():
                    def unit(q, c):
                        attend(2, 2 * (nb - 4) + q)
                        return c

                    lax.fori_loop(0, 2, unit, 0)

            if t < 2:
                hand_on(t + 1, nb)
            return c

        lax.fori_loop(0, 8, out_block, 0)
        if t == 0:
            def sent(n, c):
                qkv_send(48 + n).wait_send()
                return c

            lax.fori_loop(0, 21, sent, 0)
            r_out.wait_recv()

            def back(n, c):
                for f in x_tile(n):
                    f.start()
                return c

            lax.fori_loop(0, 24, back, 0)

    x_out.wait_send()
    r_out.wait_send()
    for t in range(PASSES):
        def done(s, c, t=t):
            seen_send(t, s).wait_send()
            return c

        lax.fori_loop(1, 8, done, 0)

        def passed(d, c, t=t):
            forward(t, d).wait_send()
            return c

        lax.fori_loop(0, CHIPS, passed, 0)

    def last(n, c):
        keep, give = put(n)
        keep.wait()
        give.wait_send()
        taken(n).wait_recv()
        return c

    lax.fori_loop(0, 24, last, 0)


def solution(mesh):
    def step(x, gain, wq, wk, wv, wo):
        chip = lax.axis_index("sp") // 2
        place = chip * TOK + jnp.arange(TOK)
        half = HEAD // 2
        angle = place.astype(jnp.float32)[:, None] * THETA ** (-jnp.arange(half, dtype=jnp.float32) / half)
        cos, sin = jnp.cos(angle), jnp.sin(angle)
        cos, sin = jnp.concatenate([cos, cos], 1), jnp.concatenate([-sin, sin], 1)
        bf, f32 = jnp.bfloat16, jnp.float32
        dma, vmem, hbm = pltpu.SemaphoreType.DMA, pl.BlockSpec(memory_space=pltpu.VMEM), pl.BlockSpec(memory_space=pl.ANY)
        return pl.pallas_call(
            _kernel,
            out_shape=[jax.ShapeDtypeStruct(x.shape, bf), jax.ShapeDtypeStruct((x.shape[0], HALF), bf)],
            in_specs=[hbm, vmem, vmem, vmem, hbm, hbm, hbm, hbm],
            out_specs=[hbm, hbm],
            scratch_shapes=[
                pltpu.VMEM((TOK, D), bf),
                pltpu.VMEM((SLOTS, 48, W, W), bf),
                pltpu.VMEM((PASSES, 3, CHIPS, TOK, W), bf),
                pltpu.VMEM((2, TOK, W), bf),
                pltpu.VMEM((25, TOK, W), bf),
                pltpu.VMEM((PASSES, 16, TOK, W), bf),
                pltpu.VMEM((24, TOK, W), f32),
                pltpu.VMEM((2, 2, 1, TOK), f32),
                pltpu.VMEM((2, 2, HEAD + 8, TOK), f32),
                dma((SLOTS, 3)), dma((2,)), dma((2,)), dma((2,)), dma((24,)), dma((9, CHIPS)), dma((PASSES, CHIPS)), dma((PASSES, CHIPS)),
                dma((PASSES, CHIPS)), dma((PASSES, CHIPS)), dma((24,)), dma((24,)), dma((24,)), dma((24, 2)),
            ],
            compiler_params=pltpu.CompilerParams(collective_id=0, has_side_effects=True, vmem_limit_bytes=67043328),
            name="layer",
        )(x, gain.reshape(D // 128, 128), cos, sin, *(w.reshape(48, W, D) for w in (wq, wk, wv)), wo.reshape(16, 3, W, D))[0]

    tokens, whole = P(("dp", "sp"), None), P(None, None)
    return jax.shard_map(
        step,
        mesh=mesh,
        in_specs=(tokens, P(None), whole, whole, whole, whole),
        out_specs=tokens,
        check_vma=False,
    )
```
